32 devices in a mesh: seq: 8 (over z, y), vocab: 4 (over x, core).
Axes of the slice: x: 2, y: 2, z: 4, core: 2. Of those that a mesh axis runs over, the one named last changes fastest.
Arguments:
- hidden: bfloat16 [768, 3584], P('seq', 'vocab'), may hold values from -40 to 40
- lm_head: bfloat16 [3584, 152064], P(None, ('seq', 'vocab')), may hold values from -1 to 1
- positions: int32 [768], replicated, may hold values from 0 to 767, as said below
- vocab_limits: int32 [768], replicated, may hold values from 76032 to 152064
- loss_mask: int32 [768], P('seq'), may hold values 0 or 1
Outputs:
- token_entropy: float32 [768], P('seq')
- mean_entropy: float32 [], replicated
The draws below stay inside these ranges and needn't reach their ends.
Inputs may be any that keep to these rules, and one draw needn't show every extreme that they name: A permutation of the positions 0 to 767: the response is cut into 16 blocks of 48 consecutive positions; rows i * 96 to i * 96 + 96 // 2 - 1 hold the positions of block i, the next 48 rows those of block 15 - i, in any order within a block.
All inputs are finite; a program needn't handle non-finite values. No bound on the sum of `loss_mask` on one device may be relied on, other than what follows from the above.
Results may differ from the reference program's by a relative error of at most 0.0003.
Values may be sent and summed in bfloat16 or wider, within the bound.
No kernel may reach another device: no remote copies, remote signals or barrier semaphores. Data moves between devices by JAX's collectives and lax.ppermute only.
A program may use at most 128 MiB of HBM per device.

```python
import math
import jax
import jax.numpy as jnp
from jax import lax

D = 3584
VOCAB = 152064
TOK_DEV = 96
TOKENS = 768


def shared_weights(key):
    return jax.random.normal(jax.random.fold_in(key, 11), (D, VOCAB), jnp.float32) / math.sqrt(D)


def draw_lm_head(key, part):
    return shared_weights(key).astype(jnp.bfloat16)


def draw_positions(key, part):
    groups = TOKENS // TOK_DEV
    half = TOK_DEV // 2
    block_keys = jax.random.split(jax.random.fold_in(key, 21), 2 * groups)
    inner = jax.vmap(lambda one_key: jax.random.permutation(one_key, half))(block_keys).astype(jnp.int32)
    first_block = jnp.arange(groups, dtype=jnp.int32)
    second_block = 2 * groups - 1 - first_block
    rows = jnp.stack([first_block[:, None] * half + inner[first_block], second_block[:, None] * half + inner[second_block]], axis=1)
    return rows.reshape(TOKENS).astype(jnp.int32)


def draw_hidden(key, part):
    values = 3.0 * jax.random.normal(jax.random.fold_in(key, 12), (TOKENS, D), jnp.float32)
    return jnp.clip(values, -40.0, 40.0).astype(jnp.bfloat16)


def touch_ends(drawn, rng, least, largest):
    shape = drawn.shape
    place = [jax.random.randint(jax.random.fold_in(rng, axis), (), 0, shape[axis]) for axis in range(len(shape))]
    drawn = drawn.at[tuple(place)].set(least)
    longest = shape.index(max(shape))
    place[longest] = (place[longest] + 1) % shape[longest]
    return drawn.at[tuple(place)].set(largest)


def setup_inputs(seed: int = 0) -> dict:
    key_of = jax.random.split(jax.random.key(seed), 6)
    return {
        "hidden": draw_hidden(jax.random.fold_in(key_of[5], 71), 0),
        "lm_head": draw_lm_head(jax.random.fold_in(key_of[5], 71), 0),
        "positions": draw_positions(jax.random.fold_in(key_of[5], 71), 0),
        "vocab_limits": touch_ends(jax.random.randint(key_of[3], (TOKENS,), VOCAB // 2, VOCAB + 1), jax.random.fold_in(key_of[3], 1), VOCAB // 2, VOCAB).astype(jnp.int32),
        "loss_mask": touch_ends((jax.random.randint(key_of[4], (TOKENS,), 0, 4) < 3).astype(jnp.int32), jax.random.fold_in(key_of[4], 1), 0, 1),
    }


masked_value = -1e30


def row_stats(logits, row_limits, first_column):
    columns = first_column + lax.iota(jnp.int32, logits.shape[1])
    allowed = columns[None, :] < row_limits[:, None]
    row_peak = jnp.max(jnp.where(allowed, logits, masked_value), axis=1)
    shifted = logits - row_peak[:, None]
    weights = jnp.where(allowed, jnp.exp(shifted), 0.0)
    row_total = jnp.sum(weights, axis=1)
    row_moment = jnp.sum(weights * jnp.where(allowed, shifted, 0.0), axis=1)
    return row_peak, row_total, row_moment


def reference(hidden, lm_head, positions, vocab_limits, loss_mask):
    def block_entropy(inputs):
        block_rows, limits_here = inputs
        logits = jnp.dot(block_rows, lm_head, preferred_element_type=jnp.float32)
        row_peak, row_total, row_moment = row_stats(logits, limits_here, 0)
        return jnp.log(row_total) - row_moment / row_total

    entropy_rows = lax.map(block_entropy, (hidden.reshape(-1, TOK_DEV, D), vocab_limits.reshape(-1, TOK_DEV)))
    token_entropy = jnp.zeros((TOKENS,), jnp.float32).at[positions].set(entropy_rows.reshape(-1))
    mask_float = loss_mask.astype(jnp.float32)
    mean_entropy = jnp.sum(token_entropy * mask_float) / jnp.maximum(jnp.sum(mask_float), 1.0)
    return token_entropy, mean_entropy
```

```python
import functools
import jax
import jax.numpy as jnp
from jax import lax
from jax.experimental import pallas as pl
from jax.experimental.pallas import tpu as pltpu
from jax.sharding import PartitionSpec as P

AXES = ("seq", "vocab")
NEG = -1e30
FAR = 1 << 30
VMEM_LIMIT = 60 * 2**20


def dot_t(a, b):
    return lax.dot_general(a, b, (((1,), (1,)), ((), ())), preferred_element_type=jnp.float32)


def fold(buf, rows, limits, base, peak, total, moment):
    for at in range(0, buf.shape[1], 128):
        lanes = slice(at, at + 128)
        room = limits[:, lanes] - base - lax.broadcasted_iota(jnp.int32, (8, 128), 0)
        old = peak[:, lanes]
        top = old
        for r in range(0, rows, 8):
            top = jnp.maximum(top, jnp.where(room > r, buf[r : r + 8, lanes], NEG))
        drop = old - top
        ratio = jnp.exp(drop)
        before = total[:, lanes]
        sums = [ratio * before, jnp.zeros_like(before)]
        moments = [ratio * (moment[:, lanes] + before * drop), jnp.zeros_like(before)]
        for r in range(0, rows, 8):
            shifted = jnp.where(room > r, buf[r : r + 8, lanes], NEG) - top
            weight = jnp.exp(shifted)
            side = r // 8 % 2
            sums[side] = sums[side] + weight
            moments[side] = moments[side] + weight * shifted
        peak[:, lanes] = top
        total[:, lanes] = sums[0] + sums[1]
        moment[:, lanes] = moments[0] + moments[1]


def stats_kernel(half, steps, slots, width, pieces, info, limits, *refs):
    blocks, (w_hbm, out, lhs, w_buf, sem, buf0, buf1, peak, total, moment) = refs[: len(pieces)], refs[len(pieces) :]
    tile = 2 * half
    first = info[0]

    def copy(step):
        slot = step % slots if isinstance(step, int) else lax.rem(step, slots)
        row = step * tile if isinstance(step, int) else pl.multiple_of(step * tile, 16)
        return pltpu.make_async_copy(w_hbm.at[pl.ds(row, tile), :], w_buf.at[slot], sem.at[slot])

    for step in range(min(slots - 1, steps)):
        copy(step).start()
    at = 1
    for block, count in zip(blocks, pieces):
        rows, depth = block.shape[1:]
        for i in range(count):
            if depth == lhs.shape[1]:
                lhs[pl.ds(pl.multiple_of(info[at], 16), rows), :] = block[i]
            else:
                lhs[pl.ds(pl.multiple_of(info[at], 16), rows), pl.ds(pl.multiple_of(info[at + 1], 128), depth)] = block[i]
            at += 2
    peak[...] = jnp.full_like(peak, NEG)
    total[...] = jnp.zeros_like(total)
    moment[...] = jnp.zeros_like(moment)
    buf1[...] = jnp.zeros_like(buf1)
    run = (limits, peak, total, moment)

    def body(step, carry):
        slot = lax.rem(step, slots)
        copy(step).wait()

        @pl.when(step + slots - 1 < steps)
        def _():
            copy(step + slots - 1).start()

        base = first + step * tile
        buf0[...] = dot_t(w_buf[slot, :half, :], lhs[...])
        fold(buf1, half, limits, jnp.where(step == 0, FAR, base - half), peak, total, moment)
        buf1[...] = dot_t(w_buf[slot, half:, :], lhs[...])
        fold(buf0, half, limits, base, peak, total, moment)
        return carry

    lax.fori_loop(0, steps, body, 0)
    fold(buf1, half, limits, first + steps * tile - half, peak, total, moment)
    top = jnp.max(peak[...], axis=0, keepdims=True)
    drop = peak[...] - top
    ratio = jnp.exp(drop)
    out[0:1, :] = top
    out[1:2, :] = jnp.sum(ratio * total[...], axis=0, keepdims=True)
    out[2:3, :] = jnp.sum(ratio * (moment[...] + total[...] * drop), axis=0, keepdims=True)


def row_stats(info, limits, blocks, w_rows, tokens, half, steps):
    depth = w_rows.shape[1]
    slots = max(2, min(4, steps))
    pieces = tuple(b.shape[0] for b in blocks)
    wide = half * 2 * steps
    return pl.pallas_call(
        functools.partial(stats_kernel, half, steps, slots, wide, pieces),
        out_shape=jax.ShapeDtypeStruct((3, tokens), jnp.float32),
        in_specs=[pl.BlockSpec(memory_space=pltpu.SMEM)]
        + [pl.BlockSpec(memory_space=pltpu.VMEM)] * (1 + len(blocks))
        + [pl.BlockSpec(memory_space=pl.ANY)],
        out_specs=pl.BlockSpec(memory_space=pltpu.VMEM),
        scratch_shapes=[
            pltpu.VMEM((tokens, depth), jnp.bfloat16),
            pltpu.VMEM((slots, 2 * half, depth), jnp.bfloat16),
            pltpu.SemaphoreType.DMA((slots,)),
            pltpu.VMEM((half, tokens), jnp.float32),
            pltpu.VMEM((half, tokens), jnp.float32),
            pltpu.VMEM((8, tokens), jnp.float32),
            pltpu.VMEM((8, tokens), jnp.float32),
            pltpu.VMEM((8, tokens), jnp.float32),
        ],
        compiler_params=pltpu.CompilerParams(vmem_limit_bytes=VMEM_LIMIT),
        cost_estimate=pl.CostEstimate(
            flops=2 * tokens * depth * wide, bytes_accessed=2 * wide * depth, transcendentals=tokens * wide
        ),
        name="row_stats",
    )(info, limits, *blocks, w_rows)


def merge(parts):
    top = jnp.max(parts[:, 0], axis=0)
    drop = parts[:, 0] - top[None]
    ratio = jnp.exp(drop)
    return top, jnp.sum(ratio * parts[:, 1], axis=0), jnp.sum(ratio * (parts[:, 2] + parts[:, 1] * drop), axis=0)


def finish_kernel(own, parts, owner, place, entropy_out, mean_out):
    groups, _, tokens = parts.shape
    each = entropy_out.shape[1]
    top, total, moment = merge(parts[...])
    entropy = (jnp.log(total) - moment / total)[None]
    hot = lax.broadcasted_iota(jnp.int32, (each, tokens), 0) == place[...]
    mine = jnp.where(hot & (owner[...] == own[0]), entropy, 0.0)
    column = jnp.sum(mine, axis=1, keepdims=True)
    square = lax.broadcasted_iota(jnp.int32, (each, each), 0) == lax.broadcasted_iota(jnp.int32, (each, each), 1)
    entropy_out[...] = jnp.sum(jnp.where(square, column, 0.0), axis=0, keepdims=True)
    mask = parts[:, 3, :each]
    at_place = jnp.dot(mask.astype(jnp.bfloat16), hot.astype(jnp.bfloat16), preferred_element_type=jnp.float32)
    group = lax.broadcasted_iota(jnp.int32, (groups, tokens), 0)
    by_row = jnp.sum(jnp.where(group == owner[...], at_place, 0.0), axis=0, keepdims=True)
    masked = jnp.sum(entropy * by_row, axis=1, keepdims=True)
    count = jnp.sum(jnp.sum(mask, axis=1, keepdims=True), axis=0, keepdims=True)
    mean_out[...] = masked / jnp.maximum(count, 1.0)


def finish(own, parts, owner, place, each):
    return pl.pallas_call(
        finish_kernel,
        out_shape=(jax.ShapeDtypeStruct((1, each), jnp.float32), jax.ShapeDtypeStruct((1, 1), jnp.float32)),
        in_specs=[pl.BlockSpec(memory_space=pltpu.SMEM)] + [pl.BlockSpec(memory_space=pltpu.VMEM)] * 3,
        out_specs=(pl.BlockSpec(memory_space=pltpu.VMEM), pl.BlockSpec(memory_space=pltpu.VMEM)),
        name="finish",
    )(own, parts, owner, place)


def swap_table(seq, vocab, moves):
    pairs = []
    for s in range(seq):
        for v in range(vocab):
            ds, dv = moves[v % 2]
            pairs.append((s * vocab + v, (s ^ ds) * vocab + (v ^ dv)))
    return pairs


def gather_plan(seq, vocab):
    plane = vocab.bit_length() - 2
    seq_bits = seq.bit_length() - 1
    stages = [((1 << b, 0), (1 << b, 0)) for b in range(plane, seq_bits)]
    for b in range(plane):
        across, along = (0, 2 << b), (1 << b, 0)
        stages += [(across, along), (along, across)]
    return stages + [((0, 1), (0, 1))]


def gather_blocks(seq, vocab, my_seq, my_vocab, hidden):
    rows, depth = hidden.shape
    stack = hidden[None]
    places = [[(0, 0)], [(0, 0)]]
    stages = gather_plan(seq, vocab)
    for n, moves in enumerate(stages):
        held = stack
        came = lax.ppermute(held, AXES, swap_table(seq, vocab, moves))
        if n < len(stages) - 1:
            stack = jnp.concatenate([held, came], axis=0)
            places = [p + [(s ^ m[0], v ^ m[1]) for s, v in p] for p, m in zip(places, moves)]
    there = [[(s, v ^ 1) for s, v in places[1]], [(s, v ^ 1) for s, v in places[0]]]
    table = jnp.array([places[c] + there[c] for c in range(2)], jnp.int32)[my_vocab % 2]
    return [held, came], (table[:, 0] ^ my_seq) * rows, (table[:, 1] ^ my_vocab) * depth


def local(seq, vocab, hidden, lm_head, positions, vocab_limits, loss_mask):
    rows, depth = hidden.shape
    columns = lm_head.shape[1]
    tokens = positions.shape[0]
    each = loss_mask.shape[0]
    my_seq, my_vocab = lax.axis_index("seq"), lax.axis_index("vocab")
    first = (my_seq * vocab + my_vocab) * columns

    if depth % 128:
        whole = lax.all_gather(lax.all_gather(hidden, "vocab", axis=1, tiled=True), "seq", axis=0, tiled=True)
        blocks = [whole[None]]
        row_at = col_at = jnp.zeros((1,), jnp.int32)
    else:
        blocks, row_at, col_at = gather_blocks(seq, vocab, my_seq, my_vocab, hidden)
    info = jnp.concatenate([first[None], jnp.stack([row_at, col_at], axis=1).reshape(-1)]).astype(jnp.int32)

    steps = max(1, round(columns / 528))
    half = -(-columns // (steps * 16)) * 8
    w_rows = lm_head.T
    spare = 2 * half * steps - columns
    limits = jnp.minimum(vocab_limits, first + columns)
    if spare:
        w_rows = jnp.pad(w_rows, ((0, spare), (0, 0)))
    limits = jnp.broadcast_to(limits[None], (8, tokens))
    stats = row_stats(info, limits, blocks, w_rows, tokens, half, steps)

    top, total, moment = merge(lax.all_gather(stats, "vocab"))
    mask = jnp.pad(loss_mask.astype(jnp.float32), (0, tokens - each))
    sent = jnp.stack([top, total, moment, mask])
    parts = lax.all_to_all(jnp.broadcast_to(sent[None], (seq, 4, tokens)), "seq", 0, 0, tiled=True)
    entropy, mean = finish(my_seq[None].astype(jnp.int32), parts, (positions // each)[None], (positions % each)[None], each)
    return entropy.reshape(each), mean.reshape(())


def solution(mesh):
    placed = (P("seq", "vocab"), P(None, AXES), P(), P(), P("seq"))
    body = functools.partial(local, mesh.shape["seq"], mesh.shape["vocab"])
    return jax.shard_map(body, mesh=mesh, in_specs=placed, out_specs=(P("seq"), P()), check_vma=False)
```

```python
import functools
import math

import jax
import jax.numpy as jnp
from jax import lax
from jax.experimental import pallas as pl
from jax.experimental.pallas import tpu as pltpu
from jax.sharding import PartitionSpec as P


AXES = ("seq", "vocab")
NEG = -1e30
FAR = 1 << 30


def dot_t(a, b):
    return lax.dot_general(a, b, (((1,), (1,)), ((), ())), preferred_element_type=jnp.float32)


def fold(buf, rows, limits, base, peak, total, moment):
    for at in range(0, buf.shape[1], 128):
        lanes = slice(at, at + 128)
        room = limits[:, lanes] - base - lax.broadcasted_iota(jnp.int32, (8, 128), 0)
        old = peak[:, lanes]
        top = old
        for r in range(0, rows, 8):
            top = jnp.maximum(top, jnp.where(room > r, buf[r : r + 8, lanes], NEG))
        drop = old - top
        ratio = jnp.exp(drop)
        before = total[:, lanes]
        sums = [ratio * before, jnp.zeros_like(before)]
        moments = [ratio * (moment[:, lanes] + before * drop), jnp.zeros_like(before)]
        for r in range(0, rows, 8):
            shifted = jnp.where(room > r, buf[r : r + 8, lanes], NEG) - top
            weight = jnp.exp(shifted)
            side = r // 8 % 2
            sums[side] = sums[side] + weight
            moments[side] = moments[side] + weight * shifted
        peak[:, lanes] = top
        total[:, lanes] = sums[0] + sums[1]
        moment[:, lanes] = moments[0] + moments[1]


def stats_kernel(half, steps, slots, moves, info, limits, w_hbm, *refs):
    arrays, (out, lhs, w_buf, sem, buf0, buf1, peak, total, moment) = refs[:-9], refs[-9:]
    tile = 2 * half
    first = info[0]

    def copy(step):
        slot = step % slots if isinstance(step, int) else lax.rem(step, slots)
        row = step * tile if isinstance(step, int) else pl.multiple_of(step * tile, 16)
        return pltpu.make_async_copy(w_hbm.at[pl.ds(row, tile), :], w_buf.at[slot], sem.at[slot])

    for step in range(min(slots - 1, steps)):
        copy(step).start()
    at = 1
    for array, start, rows, row in moves:
        depth = arrays[array].shape[2]
        to_row = pl.multiple_of(info[at + 1], 16) if row is None else row
        block = arrays[array][info[at], start : start + rows, :]
        if depth == lhs.shape[1]:
            lhs[pl.ds(to_row, rows), :] = block
        else:
            lhs[pl.ds(to_row, rows), pl.ds(pl.multiple_of(info[at + 2], 128), depth)] = block
        at += 3
    peak[...] = jnp.full_like(peak, NEG)
    total[...] = jnp.zeros_like(total)
    moment[...] = jnp.zeros_like(moment)
    buf1[...] = jnp.zeros_like(buf1)

    def body(step, carry):
        slot = lax.rem(step, slots)
        copy(step).wait()

        @pl.when(step + slots - 1 < steps)
        def _():
            copy(step + slots - 1).start()

        base = first + step * tile
        buf0[...] = dot_t(w_buf[slot, :half, :], lhs[...])
        fold(buf1, half, limits, jnp.where(step == 0, FAR, base - half), peak, total, moment)
        buf1[...] = dot_t(w_buf[slot, half:, :], lhs[...])
        fold(buf0, half, limits, base, peak, total, moment)
        return carry

    lax.fori_loop(0, steps, body, 0)
    fold(buf1, half, limits, first + steps * tile - half, peak, total, moment)
    top = jnp.max(peak[...], axis=0, keepdims=True)
    drop = peak[...] - top
    ratio = jnp.exp(drop)
    out[0:1, :] = top
    out[1:2, :] = jnp.sum(ratio * total[...], axis=0, keepdims=True)
    out[2:3, :] = jnp.sum(ratio * (moment[...] + total[...] * drop), axis=0, keepdims=True)


def row_numbers(first, moves):
    numbers = [first]
    for _, index, _, _, row, column in moves:
        numbers += [index, row, column]
    return jnp.stack([jnp.asarray(n, jnp.int32) for n in numbers])


def row_stats(info, limits, arrays, moves, w_rows, half, steps, limit):
    depth = w_rows.shape[1]
    tokens = limits.shape[1]
    fixed = tuple((m[0], m[2], m[3], m[4] if isinstance(m[4], int) else None) for m in moves)
    wide = half * 2 * steps
    slots = max(2, min(4, steps))
    return pl.pallas_call(
        functools.partial(stats_kernel, half, steps, slots, fixed),
        out_shape=jax.ShapeDtypeStruct((3, tokens), jnp.float32),
        in_specs=[pl.BlockSpec(memory_space=pltpu.SMEM), pl.BlockSpec(memory_space=pltpu.VMEM), pl.BlockSpec(memory_space=pl.ANY)]
        + [pl.BlockSpec(memory_space=pltpu.VMEM)] * len(arrays),
        out_specs=pl.BlockSpec(memory_space=pltpu.VMEM),
        scratch_shapes=[
            pltpu.VMEM((tokens, depth), jnp.bfloat16),
            pltpu.VMEM((slots, 2 * half, depth), jnp.bfloat16),
            pltpu.SemaphoreType.DMA((slots,)),
            pltpu.VMEM((half, tokens), jnp.float32),
            pltpu.VMEM((half, tokens), jnp.float32),
            pltpu.VMEM((8, tokens), jnp.float32),
            pltpu.VMEM((8, tokens), jnp.float32),
            pltpu.VMEM((8, tokens), jnp.float32),
        ],
        compiler_params=pltpu.CompilerParams(vmem_limit_bytes=limit),
        cost_estimate=pl.CostEstimate(
            flops=2 * tokens * depth * wide, bytes_accessed=2 * wide * depth, transcendentals=tokens * wide
        ),
        name="row_stats",
    )(info, limits, w_rows, *arrays)


def merge(parts):
    top = jnp.max(parts[:, 0], axis=0)
    drop = parts[:, 0] - top[None]
    ratio = jnp.exp(drop)
    return top, jnp.sum(ratio * parts[:, 1], axis=0), jnp.sum(ratio * (parts[:, 2] + parts[:, 1] * drop), axis=0)


def finish_kernel(own, parts, owner, place, entropy_out, mean_out):
    groups, _, tokens = parts.shape
    each = entropy_out.shape[1]
    _, total, moment = merge(parts[...])
    entropy = (jnp.log(total) - moment / total)[None]
    hot = lax.broadcasted_iota(jnp.int32, (each, tokens), 0) == place[...]
    mine = jnp.where(hot & (owner[...] == own[0]), entropy, 0.0)
    column = jnp.sum(mine, axis=1, keepdims=True)
    square = lax.broadcasted_iota(jnp.int32, (each, each), 0) == lax.broadcasted_iota(jnp.int32, (each, each), 1)
    entropy_out[...] = jnp.sum(jnp.where(square, column, 0.0), axis=0, keepdims=True)
    mask = parts[:, 3, :each]
    at_place = jnp.dot(mask.astype(jnp.bfloat16), hot.astype(jnp.bfloat16), preferred_element_type=jnp.float32)
    group = lax.broadcasted_iota(jnp.int32, (groups, tokens), 0)
    by_row = jnp.sum(jnp.where(group == owner[...], at_place, 0.0), axis=0, keepdims=True)
    masked = jnp.sum(entropy * by_row, axis=1, keepdims=True)
    count = jnp.sum(jnp.sum(mask, axis=1, keepdims=True), axis=0, keepdims=True)
    mean_out[...] = masked / jnp.maximum(count, 1.0)


def finish(own, parts, owner, place, each):
    return pl.pallas_call(
        finish_kernel,
        out_shape=(jax.ShapeDtypeStruct((1, each), jnp.float32), jax.ShapeDtypeStruct((1, 1), jnp.float32)),
        in_specs=[pl.BlockSpec(memory_space=pltpu.SMEM)] + [pl.BlockSpec(memory_space=pltpu.VMEM)] * 3,
        out_specs=(pl.BlockSpec(memory_space=pltpu.VMEM), pl.BlockSpec(memory_space=pltpu.VMEM)),
        name="finish",
    )(own, parts, owner, place)


def permute(seq, vocab, array, moves):
    pairs = []
    for s in range(seq):
        for v in range(vocab):
            ds, dv = moves[v % 2]
            pairs.append((s * vocab + v, (s ^ ds) * vocab + (v ^ dv)))
    return lax.ppermute(array, AXES, pairs)


def both(ds, dv):
    return ((ds, dv), (ds, dv))


def xor_blocks(array, groups, me):
    shape = array.shape
    bit = 1
    while bit < groups:
        halves = array.reshape(shape[:-1] + (groups // (2 * bit), 2, bit * (shape[-1] // groups)))
        array = jnp.where(me & bit, halves[..., ::-1, :].reshape(shape), array)
        bit *= 2
    return array


def overlapped(seq, vocab, my_seq, my_vocab, first, hidden, limits, w_rows, half, steps):
    rows, depth = hidden.shape
    tokens = rows * seq
    core = my_vocab % 2
    swap = functools.partial(permute, seq, vocab)
    x_or_y, y_or_x, cores = ((0, 2), (1, 0)), ((1, 0), (0, 2)), both(0, 1)
    own = hidden[None]
    limits = jnp.broadcast_to(xor_blocks(limits, seq, my_seq)[None], (8, tokens))
    ready = 4 * rows // 256 * 256
    early, late = [], []
    for side in range(2):
        c = core ^ side
        for j in range(2):
            for i in range(2):
                index = jnp.where(c == 0, 2 * j + i, j + 2 * i)
                column = ((my_vocab ^ (2 * i)) // 2 * 2 + c) * depth
                early.append((side, index, 0, rows, j * rows, column))
                row = (2 + j) * rows
                cut = min(max(ready - row, 0), rows)
                if cut:
                    early.append((2 + side, index, 0, cut, row, column))
                if cut < rows:
                    late.append((side, index, cut, rows - cut, row + cut - ready, column))
        for part in range(4):
            j, i = ((0, 0), (0, 1), (1, 0), (1, 1))[part]
            for k in range(seq // 2 - 2):
                column = ((my_vocab ^ (2 * i)) // 2 * 2 + c) * depth
                late.append((2 + 4 * side + part, k, 0, rows, (2 * (k + 2) + j) * rows - ready, column))
    early_info, late_info = row_numbers(first, early), row_numbers(first, late)
    early_limits, late_limits = limits[:, :ready], limits[:, ready:]

    near = swap(own, both(2, 0))
    own_x = swap(own, x_or_y)
    own_w = swap(own, y_or_x)
    far = []
    for k in range(2, seq // 2):
        far.append(swap(own, both(2 * k, 0)))
    tables = (early_info, late_info, early_limits, late_limits)
    own_x, (early_info, late_info, early_limits, late_limits) = lax.optimization_barrier((own_x, tables))
    own_d = swap(own_x, y_or_x)
    near_x = swap(near, x_or_y)
    near_w = swap(near, y_or_x)
    near_d = swap(near_x, y_or_x)
    mine = jnp.concatenate([own, own_x, own_w, own_d], axis=0)
    theirs = swap(mine, cores)
    near_mine = jnp.concatenate([near, near_x, near_w, near_d], axis=0)
    near_theirs = swap(near_mine, cores)
    far_parts = [jnp.concatenate(far, axis=0)]
    for move in (both(0, 2), both(1, 0), both(1, 2)):
        far_parts.append(swap(far_parts[0], move))
    far_theirs = []
    for part in far_parts:
        far_theirs.append(swap(part, cores))

    done = row_stats(
        early_info, early_limits, [mine, theirs, near_mine, near_theirs], early, w_rows, half, steps, 30 * 2**20
    )
    arrays = [near_mine, near_theirs, *far_parts, *far_theirs]
    rest = row_stats(late_info, late_limits, arrays, late, w_rows, half, steps, 30 * 2**20)
    return jnp.concatenate([done, rest], axis=1)


def local(seq, vocab, hidden, lm_head, positions, vocab_limits, loss_mask):
    _, depth = hidden.shape
    columns = lm_head.shape[1]
    tokens = positions.shape[0]
    each = loss_mask.shape[0]
    my_seq, my_vocab = lax.axis_index("seq"), lax.axis_index("vocab")
    first = (my_seq * vocab + my_vocab) * columns
    steps = max(1, round(columns / 528))
    half = -(-columns // (steps * 16)) * 8
    w_rows = lm_head.T
    spare = 2 * half * steps - columns
    if spare:
        w_rows = jnp.pad(w_rows, ((0, spare), (0, 0)))
    limits = jnp.minimum(vocab_limits, first + columns)
    if depth % 128 == 0 and vocab // 2 == 2 and seq >= 8:
        stats = overlapped(seq, vocab, my_seq, my_vocab, first, hidden, limits, w_rows, half, steps)
    else:
        whole = lax.all_gather(lax.all_gather(hidden, "vocab", axis=1, tiled=True), "seq", axis=0, tiled=True)
        part = math.gcd(tokens, 512)
        stats = jnp.concatenate(
            [
                row_stats(
                    row_numbers(first, [(0, 0, 0, part, 0, 0)]),
                    jnp.broadcast_to(limits[None, at : at + part], (8, part)),
                    [whole[None, at : at + part]],
                    [(0, 0, 0, part, 0, 0)],
                    w_rows,
                    half,
                    steps,
                    40 * 2**20,
                )
                for at in range(0, tokens, part)
            ],
            axis=1,
        )
        stats = xor_blocks(stats, seq, my_seq)

    top, total, moment = merge(lax.all_gather(stats, "vocab"))
    mask = jnp.pad(loss_mask.astype(jnp.float32), (0, tokens - each))
    sent = xor_blocks(jnp.stack([top, total, moment]), seq, my_seq)
    sent = jnp.concatenate([sent, mask[None]], axis=0)
    parts = lax.all_to_all(jnp.broadcast_to(sent[None], (seq, 4, tokens)), "seq", 0, 0, tiled=True)
    entropy, mean = finish(my_seq[None].astype(jnp.int32), parts, (positions // each)[None], (positions % each)[None], each)
    return entropy.reshape(each), mean.reshape(())


def solution(mesh):
    placed = (P("seq", "vocab"), P(None, AXES), P(), P(), P("seq"))

    def body(*args):
        return local(mesh.shape["seq"], mesh.shape["vocab"], *args)

    return jax.shard_map(body, mesh=mesh, in_specs=placed, out_specs=(P("seq"), P()), check_vma=False)
```

```python
import functools
import math

import jax
import jax.numpy as jnp
from jax import lax
from jax.experimental import pallas as pl
from jax.experimental.pallas import tpu as pltpu
from jax.sharding import PartitionSpec as P


AXES = ("seq", "vocab")
NEG = -1e30
FAR = 1 << 30


def dot_t(a, b):
    return lax.dot_general(a, b, (((1,), (1,)), ((), ())), preferred_element_type=jnp.float32)


def fold(buf, rows, limits, base, peak, total, moment):
    for at in range(0, buf.shape[1], 128):
        lanes = slice(at, at + 128)
        room = limits[:, lanes] - base - lax.broadcasted_iota(jnp.int32, (8, 128), 0)
        old = peak[:, lanes]
        top = old
        for r in range(0, rows, 8):
            top = jnp.maximum(top, jnp.where(room > r, buf[r : r + 8, lanes], NEG))
        drop = old - top
        ratio = jnp.exp(drop)
        before = total[:, lanes]
        sums = [ratio * before, jnp.zeros_like(before)]
        moments = [ratio * (moment[:, lanes] + before * drop), jnp.zeros_like(before)]
        for r in range(0, rows, 8):
            shifted = jnp.where(room > r, buf[r : r + 8, lanes], NEG) - top
            weight = jnp.exp(shifted)
            side = r // 8 % 2
            sums[side] = sums[side] + weight
            moments[side] = moments[side] + weight * shifted
        peak[:, lanes] = top
        total[:, lanes] = sums[0] + sums[1]
        moment[:, lanes] = moments[0] + moments[1]


def stats_kernel(half, steps, slots, paired, moves, info, limits, w_hbm, *refs):
    arrays, (out, lhs, w_buf, sem, buf0, buf1, peak, total, moment) = refs[:-9], refs[-9:]
    tile = 2 * half
    first = info[0]

    def copy(step):
        slot = step % slots if isinstance(step, int) else lax.rem(step, slots)
        row = step * tile if isinstance(step, int) else pl.multiple_of(step * tile, 16)
        return pltpu.make_async_copy(w_hbm.at[pl.ds(row, tile), :], w_buf.at[slot], sem.at[slot])

    for step in range(min(slots - 1, steps)):
        copy(step).start()
    at = 1
    for array, start, rows, row in moves:
        depth = arrays[array].shape[2]
        to_row = pl.multiple_of(info[at + 1], 16) if row is None else row
        block = arrays[array][info[at], start : start + rows, :]
        if depth == lhs.shape[1]:
            lhs[pl.ds(to_row, rows), :] = block
        else:
            lhs[pl.ds(to_row, rows), pl.ds(pl.multiple_of(info[at + 2], 128), depth)] = block
        at += 3
    peak[...] = jnp.full_like(peak, NEG)
    total[...] = jnp.zeros_like(total)
    moment[...] = jnp.zeros_like(moment)

    def arrive(step):
        copy(step).wait()
        if isinstance(step, int):
            if step + slots - 1 < steps:
                copy(step + slots - 1).start()
        else:

            @pl.when(step + slots - 1 < steps)
            def _():
                copy(step + slots - 1).start()

        return step % slots if isinstance(step, int) else lax.rem(step, slots)

    if paired:
        buf0[...] = dot_t(w_buf[arrive(0)], lhs[...])

        def body(pair, carry):
            step = 2 * pair
            buf1[...] = dot_t(w_buf[arrive(step + 1)], lhs[...])
            fold(buf0, tile, limits, first + step * tile, peak, total, moment)
            buf0[...] = dot_t(w_buf[arrive(step + 2)], lhs[...])
            fold(buf1, tile, limits, first + (step + 1) * tile, peak, total, moment)
            return carry

        lax.fori_loop(0, (steps - 1) // 2, body, 0)
        last = (steps - 1) // 2 * 2
        if last + 1 < steps:
            buf1[...] = dot_t(w_buf[arrive(last + 1)], lhs[...])
        fold(buf0, tile, limits, first + last * tile, peak, total, moment)
        if last + 1 < steps:
            fold(buf1, tile, limits, first + (last + 1) * tile, peak, total, moment)
    else:
        buf1[...] = jnp.zeros_like(buf1)

        def body(step, carry):
            slot = arrive(step)
            base = first + step * tile
            buf0[...] = dot_t(w_buf[slot, :half, :], lhs[...])
            fold(buf1, half, limits, jnp.where(step == 0, FAR, base - half), peak, total, moment)
            buf1[...] = dot_t(w_buf[slot, half:, :], lhs[...])
            fold(buf0, half, limits, base, peak, total, moment)
            return carry

        lax.fori_loop(0, steps, body, 0)
        fold(buf1, half, limits, first + steps * tile - half, peak, total, moment)
    top = jnp.max(peak[...], axis=0, keepdims=True)
    drop = peak[...] - top
    ratio = jnp.exp(drop)
    out[0:1, :] = top
    out[1:2, :] = jnp.sum(ratio * total[...], axis=0, keepdims=True)
    out[2:3, :] = jnp.sum(ratio * (moment[...] + total[...] * drop), axis=0, keepdims=True)


def row_numbers(first, moves):
    numbers = [first]
    for _, index, _, _, row, column in moves:
        numbers += [index, row, column]
    return jnp.stack([jnp.asarray(n, jnp.int32) for n in numbers])


def row_stats(info, limits, arrays, moves, w_rows, half, steps, limit):
    depth = w_rows.shape[1]
    tokens = limits.shape[1]
    fixed = tuple((m[0], m[2], m[3], m[4] if isinstance(m[4], int) else None) for m in moves)
    wide = half * 2 * steps
    slots = max(2, min(4, steps))
    paired = tokens > 256
    height = 2 * half if paired else half
    return pl.pallas_call(
        functools.partial(stats_kernel, half, steps, slots, paired, fixed),
        out_shape=jax.ShapeDtypeStruct((3, tokens), jnp.float32),
        in_specs=[pl.BlockSpec(memory_space=pltpu.SMEM), pl.BlockSpec(memory_space=pltpu.VMEM), pl.BlockSpec(memory_space=pl.ANY)]
        + [pl.BlockSpec(memory_space=pltpu.VMEM)] * len(arrays),
        out_specs=pl.BlockSpec(memory_space=pltpu.VMEM),
        scratch_shapes=[
            pltpu.VMEM((tokens, depth), jnp.bfloat16),
            pltpu.VMEM((slots, 2 * half, depth), jnp.bfloat16),
            pltpu.SemaphoreType.DMA((slots,)),
            pltpu.VMEM((height, tokens), jnp.float32),
            pltpu.VMEM((height, tokens), jnp.float32),
            pltpu.VMEM((8, tokens), jnp.float32),
            pltpu.VMEM((8, tokens), jnp.float32),
            pltpu.VMEM((8, tokens), jnp.float32),
        ],
        compiler_params=pltpu.CompilerParams(vmem_limit_bytes=limit),
        cost_estimate=pl.CostEstimate(
            flops=2 * tokens * depth * wide, bytes_accessed=2 * wide * depth, transcendentals=tokens * wide
        ),
        name="row_stats",
    )(info, limits, w_rows, *arrays)


def merge(parts):
    top = jnp.max(parts[:, 0], axis=0)
    drop = parts[:, 0] - top[None]
    ratio = jnp.exp(drop)
    return top, jnp.sum(ratio * parts[:, 1], axis=0), jnp.sum(ratio * (parts[:, 2] + parts[:, 1] * drop), axis=0)


def combine_kernel(groups, own, parts, mask, out):
    tokens = parts.shape[2]
    stats = list(merge(parts[...]))
    stats = jnp.stack([*stats, stats[0]])
    lane = lax.broadcasted_iota(jnp.int32, stats.shape, 1)
    width = tokens // groups
    bit = 1
    while bit < groups:
        step = bit * width
        low = lax.rem(lane // step, 2) == 0
        flipped = jnp.where(low, pltpu.roll(stats, tokens - step, 1), pltpu.roll(stats, step, 1))
        stats = jnp.where((own[0] & bit) != 0, flipped, stats)
        bit *= 2
    row = lax.broadcasted_iota(jnp.int32, stats.shape, 0)
    stats = jnp.where(row == 3, mask[...], stats)
    for g in range(groups):
        out[g] = stats


def combine(groups, own, parts, mask):
    tokens = parts.shape[2]
    return pl.pallas_call(
        functools.partial(combine_kernel, groups),
        out_shape=jax.ShapeDtypeStruct((groups, 4, tokens), jnp.float32),
        in_specs=[pl.BlockSpec(memory_space=pltpu.SMEM)] + [pl.BlockSpec(memory_space=pltpu.VMEM)] * 2,
        out_specs=pl.BlockSpec(memory_space=pltpu.VMEM),
        name="combine",
    )(own, parts, mask)


def finish_kernel(own, parts, owner, place, entropy_out, mean_out):
    groups, _, tokens = parts.shape
    each = entropy_out.shape[1]
    _, total, moment = merge(parts[...])
    entropy = (jnp.log(total) - moment / total)[None]
    hot = lax.broadcasted_iota(jnp.int32, (each, tokens), 0) == place[...]
    mine = jnp.where(hot & (owner[...] == own[0]), entropy, 0.0)
    column = jnp.sum(mine, axis=1, keepdims=True)
    square = lax.broadcasted_iota(jnp.int32, (each, each), 0) == lax.broadcasted_iota(jnp.int32, (each, each), 1)
    entropy_out[...] = jnp.sum(jnp.where(square, column, 0.0), axis=0, keepdims=True)
    mask = parts[:, 3, :each]
    at_place = jnp.dot(mask.astype(jnp.bfloat16), hot.astype(jnp.bfloat16), preferred_element_type=jnp.float32)
    group = lax.broadcasted_iota(jnp.int32, (groups, tokens), 0)
    by_row = jnp.sum(jnp.where(group == owner[...], at_place, 0.0), axis=0, keepdims=True)
    masked = jnp.sum(entropy * by_row, axis=1, keepdims=True)
    count = jnp.sum(jnp.sum(mask, axis=1, keepdims=True), axis=0, keepdims=True)
    mean_out[...] = masked / jnp.maximum(count, 1.0)


def finish(own, parts, owner, place, each):
    return pl.pallas_call(
        finish_kernel,
        out_shape=(jax.ShapeDtypeStruct((1, each), jnp.float32), jax.ShapeDtypeStruct((1, 1), jnp.float32)),
        in_specs=[pl.BlockSpec(memory_space=pltpu.SMEM)] + [pl.BlockSpec(memory_space=pltpu.VMEM)] * 3,
        out_specs=(pl.BlockSpec(memory_space=pltpu.VMEM), pl.BlockSpec(memory_space=pltpu.VMEM)),
        name="finish",
    )(own, parts, owner, place)


def permute(seq, vocab, array, moves):
    pairs = []
    for s in range(seq):
        for v in range(vocab):
            ds, dv = moves[v % 2]
            pairs.append((s * vocab + v, (s ^ ds) * vocab + (v ^ dv)))
    return lax.ppermute(array, AXES, pairs)


def both(ds, dv):
    return ((ds, dv), (ds, dv))


def xor_blocks(array, groups, me):
    shape = array.shape
    bit = 1
    while bit < groups:
        halves = array.reshape(shape[:-1] + (groups // (2 * bit), 2, bit * (shape[-1] // groups)))
        array = jnp.where(me & bit, halves[..., ::-1, :].reshape(shape), array)
        bit *= 2
    return array


def overlapped(seq, vocab, my_seq, my_vocab, first, hidden, limits, w_rows, half, steps):
    rows, depth = hidden.shape
    tokens = rows * seq
    core = my_vocab % 2
    swap = functools.partial(permute, seq, vocab)
    x_or_y, y_or_x, cores = ((0, 2), (1, 0)), ((1, 0), (0, 2)), both(0, 1)
    own = hidden[None]
    limits = jnp.broadcast_to(xor_blocks(limits, seq, my_seq)[None], (8, tokens))
    ready = 4 * rows // 256 * 256
    early, late = [], []
    for side in range(2):
        c = core ^ side
        for j in range(2):
            for i in range(2):
                index = jnp.where(c == 0, 2 * j + i, j + 2 * i)
                column = ((my_vocab ^ (2 * i)) // 2 * 2 + c) * depth
                early.append((side, index, 0, rows, j * rows, column))
                row = (2 + j) * rows
                cut = min(max(ready - row, 0), rows)
                if cut:
                    early.append((2 + side, index, 0, cut, row, column))
                if cut < rows:
                    source = (10 + side, 0) if i and j else (side, index)
                    late.append((source[0], source[1], cut, rows - cut, row + cut - ready, column))
        for part in range(4):
            j, i = ((0, 0), (0, 1), (1, 0), (1, 1))[part]
            for k in range(seq // 2 - 2):
                column = ((my_vocab ^ (2 * i)) // 2 * 2 + c) * depth
                late.append((2 + 4 * side + part, k, 0, rows, (2 * (k + 2) + j) * rows - ready, column))
    early_info, late_info = row_numbers(first, early), row_numbers(first, late)
    early_limits, late_limits = limits[:, :ready], limits[:, ready:]

    near = swap(own, both(2, 0))
    own_x = swap(own, x_or_y)
    own_w = swap(own, y_or_x)
    far = []
    for k in range(2, seq // 2):
        far.append(swap(own, both(2 * k, 0)))
    tables = (early_info, late_info, early_limits, late_limits)
    own_x, (early_info, late_info, early_limits, late_limits) = lax.optimization_barrier((own_x, tables))
    own_d = swap(own_x, y_or_x)
    near_x = swap(near, x_or_y)
    near_w = swap(near, y_or_x)
    near_d = swap(near_x, y_or_x)
    mine = jnp.concatenate([own, own_x, own_w, own_d], axis=0)
    theirs = swap(mine, cores)
    near_mine = jnp.concatenate([near, near_x, near_w], axis=0)
    near_theirs = swap(near_mine, cores)
    near_theirs_d = swap(near_d, cores)
    far_parts = [jnp.concatenate(far, axis=0)]
    for move in (both(0, 2), both(1, 0), both(1, 2)):
        far_parts.append(swap(far_parts[0], move))
    far_theirs = []
    for part in far_parts:
        far_theirs.append(swap(part, cores))

    done = row_stats(
        early_info, early_limits, [mine, theirs, near_mine, near_theirs], early, w_rows, half, steps, 30 * 2**20
    )
    arrays = [near_mine, near_theirs, *far_parts, *far_theirs, near_d, near_theirs_d]
    rest = row_stats(late_info, late_limits, arrays, late, w_rows, half, steps, 30 * 2**20)
    return jnp.concatenate([done, rest], axis=1)


def local(seq, vocab, hidden, lm_head, positions, vocab_limits, loss_mask):
    _, depth = hidden.shape
    columns = lm_head.shape[1]
    tokens = positions.shape[0]
    each = loss_mask.shape[0]
    my_seq, my_vocab = lax.axis_index("seq"), lax.axis_index("vocab")
    first = (my_seq * vocab + my_vocab) * columns
    steps = max(1, round(columns / 528))
    half = -(-columns // (steps * 16)) * 8
    w_rows = lm_head.T
    spare = 2 * half * steps - columns
    if spare:
        w_rows = jnp.pad(w_rows, ((0, spare), (0, 0)))
    limits = jnp.minimum(vocab_limits, first + columns)
    if depth % 128 == 0 and vocab // 2 == 2 and seq >= 8:
        stats = overlapped(seq, vocab, my_seq, my_vocab, first, hidden, limits, w_rows, half, steps)
    else:
        whole = lax.all_gather(lax.all_gather(hidden, "vocab", axis=1, tiled=True), "seq", axis=0, tiled=True)
        part = math.gcd(tokens, 512)
        stats = jnp.concatenate(
            [
                row_stats(
                    row_numbers(first, [(0, 0, 0, part, 0, 0)]),
                    jnp.broadcast_to(limits[None, at : at + part], (8, part)),
                    [whole[None, at : at + part]],
                    [(0, 0, 0, part, 0, 0)],
                    w_rows,
                    half,
                    steps,
                    40 * 2**20,
                )
                for at in range(0, tokens, part)
            ],
            axis=1,
        )
        stats = xor_blocks(stats, seq, my_seq)

    own = my_seq[None].astype(jnp.int32)
    mask = jnp.pad(loss_mask.astype(jnp.float32), (0, tokens - each))[None]
    sent = combine(seq, own, lax.all_gather(stats, "vocab"), mask)
    parts = lax.all_to_all(sent, "seq", 0, 0, tiled=True)
    entropy, mean = finish(own, parts, (positions // each)[None], (positions % each)[None], each)
    return entropy.reshape(each), mean.reshape(())


def solution(mesh):
    placed = (P("seq", "vocab"), P(None, AXES), P(), P(), P("seq"))

    def body(*args):
        return local(mesh.shape["seq"], mesh.shape["vocab"], *args)

    return jax.shard_map(body, mesh=mesh, in_specs=placed, out_specs=(P("seq"), P()), check_vma=False)
```

```python
import functools
import math

import jax
import jax.numpy as jnp
from jax import lax
from jax.experimental import pallas as pl
from jax.experimental.pallas import tpu as pltpu
from jax.sharding import PartitionSpec as P


AXES = ("seq", "vocab")
NEG = -1e30
FAR = 1 << 30


def dot_t(a, b):
    return lax.dot_general(a, b, (((1,), (1,)), ((), ())), preferred_element_type=jnp.float32)


def fold(buf, rows, limits, base, peak, total, moment):
    for at in range(0, buf.shape[1], 128):
        lanes = slice(at, at + 128)
        room = limits[:, lanes] - base - lax.broadcasted_iota(jnp.int32, (8, 128), 0)
        old = peak[:, lanes]
        top = old
        for r in range(0, rows, 8):
            top = jnp.maximum(top, jnp.where(room > r, buf[r : r + 8, lanes], NEG))
        drop = old - top
        ratio = jnp.exp(drop)
        before = total[:, lanes]
        sums = [ratio * before, jnp.zeros_like(before)]
        moments = [ratio * (moment[:, lanes] + before * drop), jnp.zeros_like(before)]
        for r in range(0, rows, 8):
            shifted = jnp.where(room > r, buf[r : r + 8, lanes], NEG) - top
            weight = jnp.exp(shifted)
            side = r // 8 % 2
            sums[side] = sums[side] + weight
            moments[side] = moments[side] + weight * shifted
        peak[:, lanes] = top
        total[:, lanes] = sums[0] + sums[1]
        moment[:, lanes] = moments[0] + moments[1]


def stats_kernel(half, steps, slots, paired, moves, info, limits, w_hbm, *refs):
    arrays, (out, lhs, w_buf, sem, buf0, buf1, peak, total, moment) = refs[:-9], refs[-9:]
    tile = 2 * half
    first = info[0]

    def copy(step):
        slot = step % slots if isinstance(step, int) else lax.rem(step, slots)
        row = step * tile if isinstance(step, int) else pl.multiple_of(step * tile, 16)
        return pltpu.make_async_copy(w_hbm.at[pl.ds(row, tile), :], w_buf.at[slot], sem.at[slot])

    for step in range(min(slots - 1, steps)):
        copy(step).start()
    at = 1
    for array, start, rows, row in moves:
        depth = arrays[array].shape[2]
        to_row = pl.multiple_of(info[at + 1], 16) if row is None else row
        block = arrays[array][info[at], start : start + rows, :]
        if depth == lhs.shape[1]:
            lhs[pl.ds(to_row, rows), :] = block
        else:
            lhs[pl.ds(to_row, rows), pl.ds(pl.multiple_of(info[at + 2], 128), depth)] = block
        at += 3
    peak[...] = jnp.full_like(peak, NEG)
    total[...] = jnp.zeros_like(total)
    moment[...] = jnp.zeros_like(moment)

    def arrive(step):
        copy(step).wait()
        if isinstance(step, int):
            if step + slots - 1 < steps:
                copy(step + slots - 1).start()
        else:

            @pl.when(step + slots - 1 < steps)
            def _():
                copy(step + slots - 1).start()

        return step % slots if isinstance(step, int) else lax.rem(step, slots)

    if paired:
        buf0[...] = dot_t(w_buf[arrive(0)], lhs[...])

        def body(pair, carry):
            step = 2 * pair
            buf1[...] = dot_t(w_buf[arrive(step + 1)], lhs[...])
            fold(buf0, tile, limits, first + step * tile, peak, total, moment)
            buf0[...] = dot_t(w_buf[arrive(step + 2)], lhs[...])
            fold(buf1, tile, limits, first + (step + 1) * tile, peak, total, moment)
            return carry

        lax.fori_loop(0, (steps - 1) // 2, body, 0)
        last = (steps - 1) // 2 * 2
        if last + 1 < steps:
            buf1[...] = dot_t(w_buf[arrive(last + 1)], lhs[...])
        fold(buf0, tile, limits, first + last * tile, peak, total, moment)
        if last + 1 < steps:
            fold(buf1, tile, limits, first + (last + 1) * tile, peak, total, moment)
    else:
        buf1[...] = jnp.zeros_like(buf1)

        def body(step, carry):
            slot = arrive(step)
            base = first + step * tile
            buf0[...] = dot_t(w_buf[slot, :half, :], lhs[...])
            fold(buf1, half, limits, jnp.where(step == 0, FAR, base - half), peak, total, moment)
            buf1[...] = dot_t(w_buf[slot, half:, :], lhs[...])
            fold(buf0, half, limits, base, peak, total, moment)
            return carry

        lax.fori_loop(0, steps, body, 0)
        fold(buf1, half, limits, first + steps * tile - half, peak, total, moment)
    top = jnp.max(peak[...], axis=0, keepdims=True)
    drop = peak[...] - top
    ratio = jnp.exp(drop)
    out[0:1, :] = top
    out[1:2, :] = jnp.sum(ratio * total[...], axis=0, keepdims=True)
    out[2:3, :] = jnp.sum(ratio * (moment[...] + total[...] * drop), axis=0, keepdims=True)


def row_numbers(first, moves):
    numbers = [first]
    for _, index, _, _, row, column in moves:
        numbers += [index, row, column]
    return jnp.stack([jnp.asarray(n, jnp.int32) for n in numbers])


def row_stats(info, limits, arrays, moves, w_rows, half, steps, limit):
    depth = w_rows.shape[1]
    tokens = limits.shape[1]
    fixed = tuple((m[0], m[2], m[3], m[4] if isinstance(m[4], int) else None) for m in moves)
    wide = half * 2 * steps
    slots = max(2, min(4, steps))
    paired = tokens > 256
    height = 2 * half if paired else half
    return pl.pallas_call(
        functools.partial(stats_kernel, half, steps, slots, paired, fixed),
        out_shape=jax.ShapeDtypeStruct((3, tokens), jnp.float32),
        in_specs=[pl.BlockSpec(memory_space=pltpu.SMEM), pl.BlockSpec(memory_space=pltpu.VMEM), pl.BlockSpec(memory_space=pl.ANY)]
        + [pl.BlockSpec(memory_space=pltpu.VMEM)] * len(arrays),
        out_specs=pl.BlockSpec(memory_space=pltpu.VMEM),
        scratch_shapes=[
            pltpu.VMEM((tokens, depth), jnp.bfloat16),
            pltpu.VMEM((slots, 2 * half, depth), jnp.bfloat16),
            pltpu.SemaphoreType.DMA((slots,)),
            pltpu.VMEM((height, tokens), jnp.float32),
            pltpu.VMEM((height, tokens), jnp.float32),
            pltpu.VMEM((8, tokens), jnp.float32),
            pltpu.VMEM((8, tokens), jnp.float32),
            pltpu.VMEM((8, tokens), jnp.float32),
        ],
        compiler_params=pltpu.CompilerParams(vmem_limit_bytes=limit),
        cost_estimate=pl.CostEstimate(
            flops=2 * tokens * depth * wide, bytes_accessed=2 * wide * depth, transcendentals=tokens * wide
        ),
        name="row_stats",
    )(info, limits, w_rows, *arrays)


def merge(parts):
    top = jnp.max(parts[:, 0], axis=0)
    drop = parts[:, 0] - top[None]
    ratio = jnp.exp(drop)
    return top, jnp.sum(ratio * parts[:, 1], axis=0), jnp.sum(ratio * (parts[:, 2] + parts[:, 1] * drop), axis=0)


def combine_kernel(groups, own, mask, *refs):
    parts, out = refs[:-1], refs[-1]
    tokens = mask.shape[1]
    stats = list(merge(jnp.stack([part[...] for part in parts])))
    stats = jnp.stack([*stats, stats[0]])
    lane = lax.broadcasted_iota(jnp.int32, stats.shape, 1)
    width = tokens // groups
    bit = 1
    while bit < groups:
        step = bit * width
        low = lax.rem(lane // step, 2) == 0
        flipped = jnp.where(low, pltpu.roll(stats, tokens - step, 1), pltpu.roll(stats, step, 1))
        stats = jnp.where((own[0] & bit) != 0, flipped, stats)
        bit *= 2
    row = lax.broadcasted_iota(jnp.int32, stats.shape, 0)
    stats = jnp.where(row == 3, mask[...], stats)
    for g in range(groups):
        out[g] = stats


def combine(groups, own, parts, mask):
    tokens = mask.shape[1]
    return pl.pallas_call(
        functools.partial(combine_kernel, groups),
        out_shape=jax.ShapeDtypeStruct((groups, 4, tokens), jnp.float32),
        in_specs=[pl.BlockSpec(memory_space=pltpu.SMEM)] + [pl.BlockSpec(memory_space=pltpu.VMEM)] * (1 + len(parts)),
        out_specs=pl.BlockSpec(memory_space=pltpu.VMEM),
        name="combine",
    )(own, mask, *parts)


def finish_kernel(own, parts, owner, place, entropy_out, mean_out):
    groups, _, tokens = parts.shape
    each = entropy_out.shape[1]
    _, total, moment = merge(parts[...])
    entropy = (jnp.log(total) - moment / total)[None]
    hot = lax.broadcasted_iota(jnp.int32, (each, tokens), 0) == place[...]
    mine = jnp.where(hot & (owner[...] == own[0]), entropy, 0.0)
    column = jnp.sum(mine, axis=1, keepdims=True)
    square = lax.broadcasted_iota(jnp.int32, (each, each), 0) == lax.broadcasted_iota(jnp.int32, (each, each), 1)
    entropy_out[...] = jnp.sum(jnp.where(square, column, 0.0), axis=0, keepdims=True)
    mask = parts[:, 3, :each]
    at_place = jnp.dot(mask.astype(jnp.bfloat16), hot.astype(jnp.bfloat16), preferred_element_type=jnp.float32)
    group = lax.broadcasted_iota(jnp.int32, (groups, tokens), 0)
    by_row = jnp.sum(jnp.where(group == owner[...], at_place, 0.0), axis=0, keepdims=True)
    masked = jnp.sum(entropy * by_row, axis=1, keepdims=True)
    count = jnp.sum(jnp.sum(mask, axis=1, keepdims=True), axis=0, keepdims=True)
    mean_out[...] = masked / jnp.maximum(count, 1.0)


def finish(own, parts, owner, place, each):
    return pl.pallas_call(
        finish_kernel,
        out_shape=(jax.ShapeDtypeStruct((1, each), jnp.float32), jax.ShapeDtypeStruct((1, 1), jnp.float32)),
        in_specs=[pl.BlockSpec(memory_space=pltpu.SMEM)] + [pl.BlockSpec(memory_space=pltpu.VMEM)] * 3,
        out_specs=(pl.BlockSpec(memory_space=pltpu.VMEM), pl.BlockSpec(memory_space=pltpu.VMEM)),
        name="finish",
    )(own, parts, owner, place)


def permute(seq, vocab, array, moves):
    pairs = []
    for s in range(seq):
        for v in range(vocab):
            ds, dv = moves[v % 2]
            pairs.append((s * vocab + v, (s ^ ds) * vocab + (v ^ dv)))
    return lax.ppermute(array, AXES, pairs)


def both(ds, dv):
    return ((ds, dv), (ds, dv))


def xor_blocks(array, groups, me):
    shape = array.shape
    bit = 1
    while bit < groups:
        halves = array.reshape(shape[:-1] + (groups // (2 * bit), 2, bit * (shape[-1] // groups)))
        array = jnp.where(me & bit, halves[..., ::-1, :].reshape(shape), array)
        bit *= 2
    return array


def overlapped(seq, vocab, my_seq, my_vocab, first, hidden, limits, w_rows, half, steps):
    rows, depth = hidden.shape
    tokens = rows * seq
    core = my_vocab % 2
    swap = functools.partial(permute, seq, vocab)
    x_or_y, y_or_x, cores = ((0, 2), (1, 0)), ((1, 0), (0, 2)), both(0, 1)
    own = hidden[None]
    limits = jnp.broadcast_to(xor_blocks(limits, seq, my_seq)[None], (8, tokens))
    ready = 4 * rows // 256 * 256
    early, late = [], []
    for side in range(2):
        c = core ^ side
        for j in range(2):
            for i in range(2):
                index = jnp.where(c == 0, 2 * j + i, j + 2 * i)
                column = ((my_vocab ^ (2 * i)) // 2 * 2 + c) * depth
                early.append((side, index, 0, rows, j * rows, column))
                row = (2 + j) * rows
                cut = min(max(ready - row, 0), rows)
                if cut:
                    early.append((2 + side, index, 0, cut, row, column))
                if cut < rows:
                    source = (10 + side, 0) if i and j else (side, index)
                    late.append((source[0], source[1], cut, rows - cut, row + cut - ready, column))
        for part in range(4):
            j, i = ((0, 0), (0, 1), (1, 0), (1, 1))[part]
            for k in range(seq // 2 - 2):
                column = ((my_vocab ^ (2 * i)) // 2 * 2 + c) * depth
                late.append((2 + 4 * side + part, k, 0, rows, (2 * (k + 2) + j) * rows - ready, column))
    early_info, late_info = row_numbers(first, early), row_numbers(first, late)
    early_limits, late_limits = limits[:, :ready], limits[:, ready:]

    near = swap(own, both(2, 0))
    own_x = swap(own, x_or_y)
    own_w = swap(own, y_or_x)
    far = []
    for k in range(2, seq // 2):
        far.append(swap(own, both(2 * k, 0)))
    tables = (early_info, late_info, early_limits, late_limits)
    own_x, (early_info, late_info, early_limits, late_limits) = lax.optimization_barrier((own_x, tables))
    own_d = swap(own_x, y_or_x)
    near_x = swap(near, x_or_y)
    near_w = swap(near, y_or_x)
    near_d = swap(near_x, y_or_x)
    mine = jnp.concatenate([own, own_x, own_w, own_d], axis=0)
    theirs = swap(mine, cores)
    near_mine = jnp.concatenate([near, near_x, near_w], axis=0)
    near_theirs = swap(near_mine, cores)
    near_theirs_d = swap(near_d, cores)
    far_parts = [jnp.concatenate(far, axis=0)]
    for move in (both(0, 2), both(1, 0), both(1, 2)):
        far_parts.append(swap(far_parts[0], move))
    far_theirs = []
    for part in far_parts:
        far_theirs.append(swap(part, cores))

    done = row_stats(
        early_info, early_limits, [mine, theirs, near_mine, near_theirs], early, w_rows, half, steps, 30 * 2**20
    )
    arrays = [near_mine, near_theirs, *far_parts, *far_theirs, near_d, near_theirs_d]
    rest = row_stats(late_info, late_limits, arrays, late, w_rows, half, steps, 30 * 2**20)
    return jnp.concatenate([done, rest], axis=1)


def local(seq, vocab, hidden, lm_head, positions, vocab_limits, loss_mask):
    _, depth = hidden.shape
    columns = lm_head.shape[1]
    tokens = positions.shape[0]
    each = loss_mask.shape[0]
    my_seq, my_vocab = lax.axis_index("seq"), lax.axis_index("vocab")
    first = (my_seq * vocab + my_vocab) * columns
    steps = max(1, round(columns / 528))
    half = -(-columns // (steps * 16)) * 8
    w_rows = lm_head.T
    spare = 2 * half * steps - columns
    if spare:
        w_rows = jnp.pad(w_rows, ((0, spare), (0, 0)))
    limits = jnp.minimum(vocab_limits, first + columns)
    if depth % 128 == 0 and vocab // 2 == 2 and seq >= 8:
        stats = overlapped(seq, vocab, my_seq, my_vocab, first, hidden, limits, w_rows, half, steps)
    else:
        whole = lax.all_gather(lax.all_gather(hidden, "vocab", axis=1, tiled=True), "seq", axis=0, tiled=True)
        part = math.gcd(tokens, 512)
        stats = jnp.concatenate(
            [
                row_stats(
                    row_numbers(first, [(0, 0, 0, part, 0, 0)]),
                    jnp.broadcast_to(limits[None, at : at + part], (8, part)),
                    [whole[None, at : at + part]],
                    [(0, 0, 0, part, 0, 0)],
                    w_rows,
                    half,
                    steps,
                    40 * 2**20,
                )
                for at in range(0, tokens, part)
            ],
            axis=1,
        )
        stats = xor_blocks(stats, seq, my_seq)

    own = my_seq[None].astype(jnp.int32)
    mask = jnp.pad(loss_mask.astype(jnp.float32), (0, tokens - each))[None]
    others = [permute(seq, vocab, stats, both(0, v)) for v in range(vocab - 1, 0, -1)]
    sent = combine(seq, own, [stats, *others], mask)
    parts = lax.all_to_all(sent, "seq", 0, 0, tiled=True)
    entropy, mean = finish(own, parts, (positions // each)[None], (positions % each)[None], each)
    return entropy.reshape(each), mean.reshape(())


def solution(mesh):
    placed = (P("seq", "vocab"), P(None, AXES), P(), P(), P("seq"))

    def body(*args):
        return local(mesh.shape["seq"], mesh.shape["vocab"], *args)

    return jax.shard_map(body, mesh=mesh, in_specs=placed, out_specs=(P("seq"), P()), check_vma=False)
```
